32 devices in a mesh: dp: 8 (over y, x, core), mp: 4 (over z).
Axes of the slice: x: 2, y: 2, z: 4, core: 2. Of those that a mesh axis runs over, the one named last changes fastest.
Arguments:
- image_tokens: bfloat16 [128, 32, 1152], P('dp'), may hold values from -6 to 6
- image_counts: int32 [8, 4], P('dp'), may hold values from 2 to 4, as said below
- image_ids: int32 [128], P('dp'), may hold values from 0 to 31
- norm_gain: float32 [1152], replicated, may hold values from 0.1 to 1.9
- norm_bias: float32 [1152], replicated, may hold values from -3 to 3
- up_weight: bfloat16 [1152, 3072], P(None, 'mp'), may hold values from -0.1875 to 0.1875
- down_weight: bfloat16 [3072, 1152], P('mp'), may hold values from -0.109375 to 0.109375
- text_rows: bfloat16 [128, 1152], P(('dp', 'mp')), may hold values from -6 to 6
- text_counts: int32 [32], P(('dp', 'mp')), may hold values from 2 to 4, as said below
- text_ids: int32 [128], replicated, may hold values from 0 to 31
- logit_scale: float32 [1], replicated, may hold values from 30 to 45
- logit_bias: float32 [1], replicated, may hold values from -8 to -5.5
Outputs:
- text_grad: float32 [128, 1152], P(('dp', 'mp'))
The draws below stay inside these ranges and needn't reach their ends.
Inputs may be any that keep to these rules, and one draw needn't show every extreme that they name: `image_counts`: entries count the valid rows among the 4 padded rows of one device's block; in every draw some block has all 4 rows valid. `text_counts`: entries count the valid rows among the 4 padded rows of one device's block; in every draw some block has all 4 rows valid.
All inputs are finite; a program needn't handle non-finite values.
Results may differ from the reference program's by a relative error of at most 0.02.
Values may be sent and summed in bfloat16 or wider, within the bound.
A program may use at most 64 MiB of HBM per device.

```python
import jax
import jax.numpy as jnp
from jax import lax

D = 1152
FF = 3072
ROWS_DEV = 4
PATCHES = 32
DATA_SHARDS = 8
WIDTH_SHARDS = 4
ROWS = 128


def valid_counts(key, count_shape):
    counts = jax.random.randint(key, count_shape, ROWS_DEV // 2, ROWS_DEV + 1)
    flattened = counts.reshape(-1)
    chosen = jax.random.randint(jax.random.fold_in(key, 11), (), 0, flattened.shape[0])
    flattened = flattened.at[chosen].set(ROWS_DEV)
    return flattened.reshape(count_shape).astype(jnp.int32)


def draw_image_counts(key, part):
    return valid_counts(jax.random.fold_in(key, 1), (DATA_SHARDS, WIDTH_SHARDS))


def draw_text_counts(key, part):
    return valid_counts(jax.random.fold_in(key, 2), (DATA_SHARDS * WIDTH_SHARDS,))


def direction_table(key):
    return jax.random.normal(jax.random.fold_in(key, 7), (ROWS // 8, D), jnp.float32)


def draw_image_tokens(key, part):
    directions = direction_table(key)
    choose = jax.random.randint(jax.random.fold_in(key, 21), (ROWS,), 0, ROWS // 8)
    strength = jax.random.uniform(jax.random.fold_in(key, 22), (ROWS,), jnp.float32, 0.35, 0.7)
    jitter = jax.random.normal(jax.random.fold_in(key, 23), (ROWS, PATCHES, D), jnp.float32)
    centers = jnp.take(directions, choose, axis=0) * strength[:, None]
    values = jitter + centers[:, None, :]
    return jnp.clip(values, -6.0, 6.0).astype(jnp.bfloat16)


def draw_text_rows(key, part):
    directions = direction_table(key)
    choose = jax.random.randint(jax.random.fold_in(key, 31), (ROWS,), 0, ROWS // 8)
    strength = jax.random.uniform(jax.random.fold_in(key, 32), (ROWS,), jnp.float32, 0.15, 0.4)
    jitter = jax.random.normal(jax.random.fold_in(key, 33), (ROWS, D), jnp.float32)
    values = jitter + jnp.take(directions, choose, axis=0) * strength[:, None]
    return jnp.clip(values, -6.0, 6.0).astype(jnp.bfloat16)


def place_ends(values, rng, smallest, top_value):
    spot = [jax.random.randint(jax.random.fold_in(rng, axis), (), 0, length) for axis, length in enumerate(values.shape)]
    longest = values.shape.index(max(values.shape))
    neighbour = spot[:longest] + [(spot[longest] + 1) % values.shape[longest]] + spot[longest + 1:]
    return values.at[tuple(spot)].set(smallest).at[tuple(neighbour)].set(top_value)


def levels(rng, dims, shards, low, high):
    factor_of, own = 1.0, jax.random.fold_in(rng, 6)
    for position, shards_of in shards:
        heights = jnp.exp(jax.random.uniform(jax.random.fold_in(own, position), (shards_of,), jnp.float32, low / len(shards), high / len(shards)))
        factor_of = factor_of * jnp.repeat(heights, dims[position] // shards_of).reshape([-1 if axis == position else 1 for axis in range(len(dims))])
    return factor_of


def normal_values(own_key, extent, deviation, bound, cuts=(), held_as=jnp.bfloat16):
    values = deviation * jax.random.normal(own_key, extent, jnp.float32)
    if cuts:
        values = values * levels(own_key, extent, cuts, -0.22, 0.18)
    return jnp.clip(values, -bound, bound).astype(held_as)


def setup_inputs(seed: int = 0) -> dict:
    key_of = jax.random.split(jax.random.key(seed), 13)
    image_tokens = draw_image_tokens(jax.random.fold_in(key_of[12], 71), 0)
    image_counts = draw_image_counts(jax.random.fold_in(key_of[12], 71), 0)
    image_ids = place_ends(jax.random.randint(key_of[2], (ROWS,), 0, ROWS // 4), jax.random.fold_in(key_of[2], 1), 0, (ROWS // 4) - 1).astype(jnp.int32)
    norm_gain = jnp.clip(1.0 + 0.18 * jax.random.normal(key_of[3], (D,), jnp.float32), 0.1, 1.9)
    norm_bias = normal_values(key_of[4], (D,), 0.5, 3.0, (), jnp.float32)
    up_weight = normal_values(key_of[5], (D, FF), D ** -0.5, 0.1875, ((1, 4),))
    down_weight = normal_values(key_of[6], (FF, D), FF ** -0.5, 0.109375, ((0, 4),))
    text_rows = draw_text_rows(jax.random.fold_in(key_of[12], 71), 0)
    text_counts = draw_text_counts(jax.random.fold_in(key_of[12], 71), 0)
    text_ids = place_ends(jax.random.randint(key_of[9], (ROWS,), 0, ROWS // 4), jax.random.fold_in(key_of[9], 1), 0, (ROWS // 4) - 1).astype(jnp.int32)
    logit_scale = jnp.clip(jax.random.uniform(key_of[10], (1,), jnp.float32, 30.0, 45.0), 30.0, 45.0)
    logit_bias = jnp.clip(jax.random.uniform(key_of[11], (1,), jnp.float32, -8.0, -5.5), -8.0, -5.5)
    return dict(image_tokens=image_tokens, image_counts=image_counts, image_ids=image_ids, norm_gain=norm_gain, norm_bias=norm_bias, up_weight=up_weight, down_weight=down_weight, text_rows=text_rows, text_counts=text_counts, text_ids=text_ids, logit_scale=logit_scale, logit_bias=logit_bias)


norm_eps = 1e-06

def layer_norm(row_values, gain_row, shift_row):
    values = row_values.astype(jnp.float32)
    center = lax.optimization_barrier(jnp.mean(values, axis=-1, keepdims=True))
    spread = lax.optimization_barrier(jnp.mean(jnp.square(values - center), axis=-1, keepdims=True))
    return (values - center) * lax.rsqrt(spread + norm_eps) * gain_row + shift_row

def unit_rows(values):
    return values * lax.rsqrt(lax.optimization_barrier(jnp.sum(values * values, axis=-1, keepdims=True)) + norm_eps)

def pool_hidden(token_block, gain_row, shift_row, up_weight):
    normed = layer_norm(token_block, gain_row, shift_row).astype(jnp.bfloat16)
    hidden = jax.nn.gelu(jnp.dot(normed, up_weight, preferred_element_type=jnp.float32)).astype(jnp.bfloat16)
    return lax.optimization_barrier(jnp.mean(hidden.astype(jnp.float32), axis=1)).astype(jnp.bfloat16)

def pair_terms(text_block, block_ids, image_emb, image_ids, image_valid, logit_mul, logit_add):
    cosines = lax.dot_general(text_block, image_emb, (((1,), (1,)), ((), ())), preferred_element_type=jnp.float32)
    logits = logit_mul * cosines + logit_add
    sign_table = jnp.where(block_ids[:, None] == image_ids[None, :], 1.0, -1.0).astype(jnp.float32)
    margin = -sign_table * logits
    weights = (image_valid[None, :] * -sign_table * jax.nn.sigmoid(margin) * logit_mul).astype(jnp.bfloat16)
    return jnp.dot(weights, image_emb, preferred_element_type=jnp.float32)

def reference(image_tokens, image_counts, image_ids, norm_gain, norm_bias, up_weight, down_weight, text_rows, text_counts, text_ids, logit_scale, logit_bias):
    token_groups = image_tokens.reshape(ROWS // ROWS_DEV, ROWS_DEV, PATCHES, D)

    def one_group(token_block):
        return pool_hidden(token_block, norm_gain, norm_bias, up_weight)
    pooled_hidden = lax.map(one_group, token_groups).reshape(ROWS, FF)
    pooled_tokens = lax.optimization_barrier(jnp.mean(image_tokens.astype(jnp.float32), axis=1))
    tower_out = pooled_tokens + jnp.dot(pooled_hidden, down_weight, preferred_element_type=jnp.float32)
    image_emb = unit_rows(tower_out).astype(jnp.bfloat16)
    text_emb = unit_rows(text_rows.astype(jnp.float32)).astype(jnp.bfloat16)
    slot_index = jnp.arange(ROWS, dtype=jnp.int32) % ROWS_DEV
    image_valid = (slot_index < jnp.repeat(image_counts.reshape(-1), ROWS_DEV, total_repeat_length=ROWS)).astype(jnp.float32)
    text_valid = (slot_index < jnp.repeat(text_counts.reshape(-1), ROWS_DEV, total_repeat_length=ROWS)).astype(jnp.float32)
    text_block_rows = ROWS_DEV * WIDTH_SHARDS
    blocks = text_emb.reshape(ROWS // text_block_rows, text_block_rows, D)
    id_blocks = text_ids.reshape(ROWS // text_block_rows, text_block_rows)
    logit_mul = logit_scale[0]
    logit_add = logit_bias[0]

    def one_block(members):
        return pair_terms(members[0], members[1], image_emb, image_ids, image_valid, logit_mul, logit_add)
    grad_rows = lax.map(one_block, (blocks, id_blocks)).reshape(ROWS, D)
    return grad_rows * text_valid[:, None]
```

```python
import functools

import jax
import jax.numpy as jnp
from jax import lax
from jax.experimental import pallas as pl
from jax.experimental.pallas import tpu as pltpu
from jax.sharding import PartitionSpec as P

norm_eps = 1e-06


def unit_rows(values):
    return values * lax.rsqrt(jnp.sum(values * values, axis=-1, keepdims=True) + norm_eps)


def gelu(x):
    inner = x * (0.7978845608028654 + (0.7978845608028654 * 0.044715) * (x * x))
    return 0.5 * x * (1.0 + jnp.tanh(inner))


def kernel(
    dp,
    mp,
    chunk,
    tokens_hbm,
    image_counts,
    image_ids,
    gain,
    shift,
    up_hbm,
    down_hbm,
    text_rows,
    text_counts,
    text_ids,
    logit_scale,
    logit_bias,
    out,
    tokens,
    up,
    down,
    pooled_tokens,
    pooled_hidden,
    text_all,
    part_send,
    part_recv,
    grad_send,
    grad_recv,
    token_sem,
    up_sem,
    down_sem,
    text_ssem,
    text_rsem,
    part_ssem,
    part_rsem,
    grad_ssem,
    grad_rsem,
):
    images, patches, width = tokens.shape
    rows_dev = text_rows.shape[0]
    chunks = images // chunk
    texts = dp * rows_dev
    my_d = lax.axis_index("dp")
    my_m = lax.axis_index("mp")

    def token_copy(c):
        part = pl.ds(c * chunk, chunk)
        return pltpu.make_async_copy(tokens_hbm.at[part], tokens.at[part], token_sem.at[c])

    def behind(axis, size, me, o):
        return {axis: lax.rem(me + (size - o), size)}

    def ahead(axis, size, me, o):
        return {axis: lax.rem(me + o, size)}

    up_copy = pltpu.make_async_copy(up_hbm, up, up_sem)
    down_copy = pltpu.make_async_copy(down_hbm, down, down_sem)
    token_copy(0).start()
    up_copy.start()
    for c in range(1, chunks):
        token_copy(c).start()
    down_copy.start()

    barrier = pltpu.get_barrier_semaphore()
    for o in range(1, mp):
        pl.semaphore_signal(barrier, inc=1, device_id=ahead("mp", mp, my_m, o))
    for o in range(1, dp):
        pl.semaphore_signal(barrier, inc=1, device_id=ahead("dp", dp, my_d, o))

    def visit(c):
        token_copy(c).wait()
        first = pl.multiple_of(c * chunk, chunk)
        block = tokens[pl.ds(first, chunk)].astype(jnp.float32)
        pooled_tokens[pl.ds(first, chunk), :] = jnp.sum(block, axis=1) * (1.0 / patches)
        values = block.reshape(chunk * patches, width)
        center = jnp.mean(values, axis=-1, keepdims=True)
        values = values - center
        spread = jnp.mean(values * values, axis=-1, keepdims=True)
        normed = values * lax.rsqrt(spread + norm_eps) * gain[...].reshape(1, -1) + shift[...].reshape(1, -1)
        normed = normed.astype(jnp.bfloat16)
        return first, normed

    def finish(first, normed):
        hidden = gelu(jnp.dot(normed, up[...], preferred_element_type=jnp.float32))
        hidden = hidden.reshape(chunk, patches, hidden.shape[-1])
        pooled_hidden[pl.ds(first, chunk), :] = jnp.sum(hidden, axis=1) * (1.0 / patches)

    def text_copy(o):
        return pltpu.make_async_remote_copy(
            src_ref=text_rows,
            dst_ref=text_all.at[o - 1],
            send_sem=text_ssem.at[o - 1],
            recv_sem=text_rsem.at[o - 1],
            device_id=ahead("dp", dp, my_d, o),
        )

    def part_copy(o):
        return pltpu.make_async_remote_copy(
            src_ref=part_send,
            dst_ref=part_recv.at[o - 1],
            send_sem=part_ssem.at[o - 1],
            recv_sem=part_rsem.at[o - 1],
            device_id=ahead("mp", mp, my_m, o),
        )

    def grad_copy(o):
        return pltpu.make_async_remote_copy(
            src_ref=grad_send.at[o - 1],
            dst_ref=grad_recv.at[o - 1],
            send_sem=grad_ssem.at[o - 1],
            recv_sem=grad_rsem.at[o - 1],
            device_id=behind("dp", dp, my_d, o),
        )

    first, normed = visit(0)
    up_copy.wait()
    finish(first, normed)
    pl.semaphore_wait(barrier, dp + mp - 2)
    for o in range(1, dp):
        text_copy(o).start()
    if chunks <= 4:
        for c in range(1, chunks):
            finish(*visit(c))
    else:

        @pl.loop(1, chunks)
        def _(c):
            finish(*visit(c))

    down_copy.wait()
    part = jnp.dot(
        pooled_hidden[...].astype(jnp.bfloat16), down[...], preferred_element_type=jnp.float32
    )
    part_send[...] = part.astype(jnp.bfloat16)
    for o in range(1, mp):
        part_copy(o).start()
    tower = part + pooled_tokens[...]

    row = lax.broadcasted_iota(jnp.int32, (texts, 1), 0)
    hop = row // rows_dev
    source = my_d - hop
    source = jnp.where(source < 0, source + dp, source)
    place = (source * mp + my_m) * rows_dev + (row - hop * rows_dev)
    id_count = text_ids.shape[1]
    column = lax.broadcasted_iota(jnp.int32, (texts, id_count), 1)
    block_ids = jnp.sum(
        jnp.where(column == place, text_ids[...], 0), axis=1, keepdims=True
    )
    slot = lax.broadcasted_iota(jnp.int32, (1, images), 1)
    group = slot // rows_dev
    counts = jnp.zeros((1, images), jnp.int32)
    for k in range(image_counts.shape[1]):
        counts = jnp.where(group == k, image_counts[:, k : k + 1], counts)
    scale = logit_scale[...].reshape(1, 1)
    sign = jnp.where(block_ids == image_ids[...], 1.0, -1.0).astype(jnp.float32)
    image_valid = (slot - group * rows_dev < counts).astype(jnp.float32)
    factor = image_valid * -sign * scale

    for o in range(1, dp):
        text_copy(o).wait_recv()
    text_emb = jnp.concatenate(
        [unit_rows(text_rows[...].astype(jnp.float32))]
        + [unit_rows(text_all[o - 1].astype(jnp.float32)) for o in range(1, dp)],
        axis=0,
    ).astype(jnp.bfloat16)

    for o in range(1, mp):
        part_copy(o).wait_recv()
        tower = tower + part_recv[o - 1].astype(jnp.float32)
    image_emb = unit_rows(tower).astype(jnp.bfloat16)
    cosines = lax.dot_general(
        text_emb, image_emb, (((1,), (1,)), ((), ())), preferred_element_type=jnp.float32
    )
    logits = scale * cosines + logit_bias[...].reshape(1, 1)
    weights = (factor * jax.nn.sigmoid(-sign * logits)).astype(jnp.bfloat16)
    grads = jnp.dot(weights, image_emb, preferred_element_type=jnp.float32)
    for o in range(1, dp):
        grad_send[o - 1] = grads[o * rows_dev : (o + 1) * rows_dev].astype(jnp.bfloat16)
        grad_copy(o).start()
    total = grads[:rows_dev]
    slots = lax.broadcasted_iota(jnp.int32, (rows_dev, 1), 0)
    text_valid = (slots < text_counts[...].reshape(1, 1)).astype(jnp.float32)
    for o in range(1, dp):
        grad_copy(o).wait_recv()
        total = total + grad_recv[o - 1].astype(jnp.float32)
    out[...] = total * text_valid
    for o in range(1, dp):
        text_copy(o).wait_send()
        grad_copy(o).wait_send()
    for o in range(1, mp):
        part_copy(o).wait_send()


def local(
    image_tokens,
    image_counts,
    image_ids,
    norm_gain,
    norm_bias,
    up_weight,
    down_weight,
    text_rows,
    text_counts,
    text_ids,
    logit_scale,
    logit_bias,
):
    dp = lax.axis_size("dp")
    mp = lax.axis_size("mp")
    images, patches, width = image_tokens.shape
    rows_dev = text_rows.shape[0]
    hidden = up_weight.shape[1]
    chunk = 8
    bf16, f32 = jnp.bfloat16, jnp.float32
    dma = pltpu.SemaphoreType.DMA
    vmem = pl.BlockSpec(memory_space=pltpu.VMEM)
    hbm = pl.BlockSpec(memory_space=pl.ANY)
    return pl.pallas_call(
        functools.partial(kernel, dp, mp, chunk),
        out_shape=jax.ShapeDtypeStruct((rows_dev, width), f32),
        in_specs=[hbm, vmem, vmem, vmem, vmem, hbm, hbm, vmem, vmem, vmem, vmem, vmem],
        out_specs=vmem,
        scratch_shapes=[
            pltpu.VMEM(image_tokens.shape, bf16),
            pltpu.VMEM(up_weight.shape, bf16),
            pltpu.VMEM(down_weight.shape, bf16),
            pltpu.VMEM((images, width), f32),
            pltpu.VMEM((images, hidden), f32),
            pltpu.VMEM((dp - 1, rows_dev, width), bf16),
            pltpu.VMEM((images, width), bf16),
            pltpu.VMEM((mp - 1, images, width), bf16),
            pltpu.VMEM((dp - 1, rows_dev, width), bf16),
            pltpu.VMEM((dp - 1, rows_dev, width), bf16),
            dma((images // chunk,)),
            dma,
            dma,
            dma((dp - 1,)),
            dma((dp - 1,)),
            dma((mp - 1,)),
            dma((mp - 1,)),
            dma((dp - 1,)),
            dma((dp - 1,)),
        ],
        compiler_params=pltpu.CompilerParams(collective_id=0, has_side_effects=True),
        name="tower_pair_grad",
    )(
        image_tokens,
        image_counts,
        image_ids.reshape(1, -1),
        norm_gain,
        norm_bias,
        up_weight,
        down_weight,
        text_rows,
        text_counts,
        text_ids.reshape(1, -1),
        logit_scale,
        logit_bias,
    )


def solution(mesh):
    placed = (
        P("dp", None, None),
        P("dp", None),
        P("dp"),
        P(),
        P(),
        P(None, "mp"),
        P("mp", None),
        P(("dp", "mp"), None),
        P(("dp", "mp")),
        P(),
        P(),
        P(),
    )
    return jax.shard_map(
        local, mesh=mesh, in_specs=placed, out_specs=P(("dp", "mp"), None), check_vma=False
    )
```

```python
import functools

import jax
import jax.numpy as jnp
from jax import lax
from jax.experimental import pallas as pl
from jax.experimental.pallas import tpu as pltpu
from jax.sharding import PartitionSpec as P

norm_eps = 1e-06


def unit_rows(values):
    return values * lax.rsqrt(jnp.sum(values * values, axis=-1, keepdims=True) + norm_eps)


def gelu(x):
    inner = x * (0.7978845608028654 + (0.7978845608028654 * 0.044715) * (x * x))
    return 0.5 * x * (1.0 + jnp.tanh(inner))


def kernel(
    dp,
    mp,
    chunk,
    tokens_hbm,
    counts_hbm,
    image_ids_hbm,
    gain_hbm,
    shift_hbm,
    up_hbm,
    down_hbm,
    text_hbm,
    text_counts_hbm,
    text_ids_hbm,
    scale_hbm,
    bias_hbm,
    out,
    tokens,
    up,
    down,
    image_counts,
    image_ids,
    gain,
    shift,
    text_rows,
    text_counts,
    text_ids,
    logit_scale,
    logit_bias,
    tower,
    pooled_hidden,
    text_all,
    part_send,
    part_recv,
    grad_send,
    grad_recv,
    token_sem,
    up_sem,
    down_sem,
    small_sem,
    text_ssem,
    text_rsem,
    part_ssem,
    part_rsem,
    grad_ssem,
    grad_rsem,
):
    images, patches, width = tokens.shape
    rows_dev = text_rows.shape[0]
    chunks = images // chunk
    texts = dp * rows_dev
    my_d = lax.axis_index("dp")
    my_m = lax.axis_index("mp")

    def token_copy(c):
        part = pl.ds(c * chunk, chunk)
        return pltpu.make_async_copy(tokens_hbm.at[part], tokens.at[part], token_sem.at[c])

    def behind(axis, size, me, o):
        return {axis: lax.rem(me + (size - o), size)}

    def ahead(axis, size, me, o):
        return {axis: lax.rem(me + o, size)}

    up_copy = pltpu.make_async_copy(up_hbm, up, up_sem)
    down_copy = pltpu.make_async_copy(down_hbm, down, down_sem)
    gain_copy = pltpu.make_async_copy(gain_hbm, gain, small_sem.at[0])
    shift_copy = pltpu.make_async_copy(shift_hbm, shift, small_sem.at[1])
    late = (
        (text_hbm, text_rows),
        (text_ids_hbm, text_ids),
        (image_ids_hbm, image_ids),
        (counts_hbm, image_counts),
        (text_counts_hbm, text_counts),
        (scale_hbm, logit_scale),
        (bias_hbm, logit_bias),
    )
    late_copies = [
        pltpu.make_async_copy(source, target, small_sem.at[2 + k])
        for k, (source, target) in enumerate(late)
    ]
    token_copy(0).start()
    gain_copy.start()
    shift_copy.start()
    up_copy.start()
    barrier = pltpu.get_barrier_semaphore()
    for o in range(1, mp):
        pl.semaphore_signal(barrier, inc=1, device_id=ahead("mp", mp, my_m, o))
    for o in range(1, dp):
        pl.semaphore_signal(barrier, inc=1, device_id=ahead("dp", dp, my_d, o))
    for c in range(1, chunks):
        token_copy(c).start()
    down_copy.start()
    for copy in late_copies:
        copy.start()

    pool_row = lax.broadcasted_iota(jnp.int32, (chunk, chunk * patches), 0)
    pool_column = lax.broadcasted_iota(jnp.int32, (chunk, chunk * patches), 1) // patches
    pool = jnp.where(pool_row == pool_column, 1.0 / patches, 0.0).astype(jnp.bfloat16)

    def visit(c):
        first = pl.multiple_of(c * chunk, chunk)
        block = tokens[pl.ds(first, chunk)].reshape(chunk * patches, width)
        tower[pl.ds(first, chunk), :] = jnp.dot(pool, block, preferred_element_type=jnp.float32)
        values = block.astype(jnp.float32)
        center = jnp.mean(values, axis=-1, keepdims=True)
        values = values - center
        spread = jnp.mean(values * values, axis=-1, keepdims=True)
        normed = (
            values * lax.rsqrt(spread + norm_eps) * gain[...].reshape(1, -1)
            + shift[...].reshape(1, -1)
        )
        return normed.astype(jnp.bfloat16)

    def finish(c, normed):
        first = pl.multiple_of(c * chunk, chunk)
        hidden = jnp.dot(normed, up[...], preferred_element_type=jnp.float32)
        hidden = gelu(hidden).astype(jnp.bfloat16)
        pooled_hidden[pl.ds(first, chunk), :] = jnp.dot(
            pool, hidden, preferred_element_type=jnp.float32
        )

    def text_copy(o):
        return pltpu.make_async_remote_copy(
            src_ref=text_hbm,
            dst_ref=text_all.at[o - 1],
            send_sem=text_ssem.at[o - 1],
            recv_sem=text_rsem.at[o - 1],
            device_id=ahead("dp", dp, my_d, o),
        )

    def part_copy(o, c):
        return pltpu.make_async_remote_copy(
            src_ref=part_send.at[c],
            dst_ref=part_recv.at[o - 1, c],
            send_sem=part_ssem.at[o - 1, c],
            recv_sem=part_rsem.at[o - 1, c],
            device_id=ahead("mp", mp, my_m, o),
        )

    def grad_copy(o):
        return pltpu.make_async_remote_copy(
            src_ref=grad_send.at[o - 1],
            dst_ref=grad_recv.at[o - 1],
            send_sem=grad_ssem.at[o - 1],
            recv_sem=grad_rsem.at[o - 1],
            device_id=behind("dp", dp, my_d, o),
        )

    def project(c):
        first = pl.multiple_of(c * chunk, chunk)
        pooled = pooled_hidden[pl.ds(first, chunk), :].astype(jnp.bfloat16)
        part = jnp.dot(pooled, down[...], preferred_element_type=jnp.float32)
        part_send[c] = part.astype(jnp.bfloat16)
        for o in range(1, mp):
            part_copy(o, c).start()
        tower[pl.ds(first, chunk), :] += part

    gain_copy.wait()
    shift_copy.wait()
    token_copy(0).wait()
    normed = visit(0)
    up_copy.wait()
    finish(0, normed)
    pl.semaphore_wait(barrier, dp + mp - 2)
    for o in range(1, dp):
        text_copy(o).start()
    if chunks <= 4:
        for c in range(1, chunks):
            token_copy(c).wait()
            normed = visit(c)
            if c == 1:
                down_copy.wait()
            project(c - 1)
            finish(c, normed)
        if chunks == 1:
            down_copy.wait()
    else:
        down_copy.wait()

        @pl.loop(1, chunks)
        def _(c):
            token_copy(c).wait()
            project(c - 1)
            finish(c, visit(c))

    project(chunks - 1)

    for copy in late_copies:
        copy.wait()
    row = lax.broadcasted_iota(jnp.int32, (texts, 1), 0)
    hop = row // rows_dev
    source = my_d - hop
    source = jnp.where(source < 0, source + dp, source)
    place = (source * mp + my_m) * rows_dev + (row - hop * rows_dev)
    id_count = text_ids.shape[1]
    column = lax.broadcasted_iota(jnp.int32, (texts, id_count), 1)
    block_ids = jnp.sum(jnp.where(column == place, text_ids[...], 0), axis=1, keepdims=True)
    slot = lax.broadcasted_iota(jnp.int32, (1, images), 1)
    group = slot // rows_dev
    counts = jnp.zeros((1, images), jnp.int32)
    for k in range(image_counts.shape[1]):
        counts = jnp.where(group == k, image_counts[:, k : k + 1], counts)
    scale = logit_scale[0]
    sign = jnp.where(block_ids == image_ids[...], 1.0, -1.0).astype(jnp.float32)
    image_valid = (slot - group * rows_dev < counts).astype(jnp.float32)
    factor = image_valid * -sign * scale

    for o in range(1, dp):
        text_copy(o).wait_recv()
    text_emb = jnp.concatenate(
        [unit_rows(text_rows[...].astype(jnp.float32))]
        + [unit_rows(text_all[o - 1].astype(jnp.float32)) for o in range(1, dp)],
        axis=0,
    ).astype(jnp.bfloat16)

    total = tower[...]
    for o in range(1, mp):
        for c in range(chunks):
            part_copy(o, c).wait_recv()
        total = total + part_recv[o - 1].astype(jnp.float32).reshape(images, width)
    image_emb = unit_rows(total).astype(jnp.bfloat16)
    cosines = lax.dot_general(
        text_emb, image_emb, (((1,), (1,)), ((), ())), preferred_element_type=jnp.float32
    )
    logits = scale * cosines + logit_bias[0]
    weights = (factor * jax.nn.sigmoid(-sign * logits)).astype(jnp.bfloat16)
    grads = jnp.dot(weights, image_emb, preferred_element_type=jnp.float32)
    for o in range(dp - 1, 0, -1):
        grad_send[o - 1] = grads[o * rows_dev : (o + 1) * rows_dev].astype(jnp.bfloat16)
        grad_copy(o).start()
    grad = grads[:rows_dev]
    slots = lax.broadcasted_iota(jnp.int32, (rows_dev, 1), 0)
    text_valid = (slots < text_counts[0]).astype(jnp.float32)
    for o in range(1, dp):
        grad_copy(o).wait_recv()
        grad = grad + grad_recv[o - 1].astype(jnp.float32)
    out[...] = grad * text_valid
    for o in range(1, dp):
        text_copy(o).wait_send()
        grad_copy(o).wait_send()
    for o in range(1, mp):
        for c in range(chunks):
            part_copy(o, c).wait_send()


def local(
    image_tokens,
    image_counts,
    image_ids,
    norm_gain,
    norm_bias,
    up_weight,
    down_weight,
    text_rows,
    text_counts,
    text_ids,
    logit_scale,
    logit_bias,
):
    dp = lax.axis_size("dp")
    mp = lax.axis_size("mp")
    images, patches, width = image_tokens.shape
    rows_dev = text_rows.shape[0]
    hidden = up_weight.shape[1]
    chunk = 8
    bf16, f32, i32 = jnp.bfloat16, jnp.float32, jnp.int32
    dma = pltpu.SemaphoreType.DMA
    vmem = pl.BlockSpec(memory_space=pltpu.VMEM)
    hbm = pl.BlockSpec(memory_space=pltpu.HBM)
    return pl.pallas_call(
        functools.partial(kernel, dp, mp, chunk),
        out_shape=pltpu.VMEM((rows_dev, width), f32),
        in_specs=[hbm] * 12,
        out_specs=vmem,
        scratch_shapes=[
            pltpu.VMEM(image_tokens.shape, bf16),
            pltpu.VMEM(up_weight.shape, bf16),
            pltpu.VMEM(down_weight.shape, bf16),
            pltpu.VMEM(image_counts.shape, i32),
            pltpu.VMEM((1, images), i32),
            pltpu.VMEM((width,), f32),
            pltpu.VMEM((width,), f32),
            pltpu.VMEM(text_rows.shape, bf16),
            pltpu.SMEM((1,), i32),
            pltpu.VMEM((1, text_ids.shape[0]), i32),
            pltpu.SMEM((1,), f32),
            pltpu.SMEM((1,), f32),
            pltpu.VMEM((images, width), f32),
            pltpu.VMEM((images, hidden), f32),
            pltpu.VMEM((dp - 1, rows_dev, width), bf16),
            pltpu.VMEM((images // chunk, chunk, width), bf16),
            pltpu.VMEM((mp - 1, images // chunk, chunk, width), bf16),
            pltpu.VMEM((dp - 1, rows_dev, width), bf16),
            pltpu.VMEM((dp - 1, rows_dev, width), bf16),
            dma((images // chunk,)),
            dma,
            dma,
            dma((9,)),
            dma((dp - 1,)),
            dma((dp - 1,)),
            dma((mp - 1, images // chunk)),
            dma((mp - 1, images // chunk)),
            dma((dp - 1,)),
            dma((dp - 1,)),
        ],
        compiler_params=pltpu.CompilerParams(collective_id=0, has_side_effects=True),
        name="tower_pair_grad",
    )(
        image_tokens,
        image_counts,
        image_ids.reshape(1, -1),
        norm_gain,
        norm_bias,
        up_weight,
        down_weight,
        text_rows,
        text_counts,
        text_ids.reshape(1, -1),
        logit_scale,
        logit_bias,
    )


def solution(mesh):
    placed = (
        P("dp", None, None),
        P("dp", None),
        P("dp"),
        P(),
        P(),
        P(None, "mp"),
        P("mp", None),
        P(("dp", "mp"), None),
        P(("dp", "mp")),
        P(),
        P(),
        P(),
    )
    return jax.shard_map(
        local, mesh=mesh, in_specs=placed, out_specs=P(("dp", "mp"), None), check_vma=False
    )
```
